32 devices in a mesh: aux: 8 (over y, x, core), pair: 4 (over z).
Axes of the slice: x: 2, y: 2, z: 4, core: 2. Of those that a mesh axis runs over, the one named last changes fastest.
Arguments:
- integrals: bfloat16 [3072, 32768], P('aux', 'pair'), may hold values from -0.15625 to 0.15625
- densities: bfloat16 [16, 32768], P(None, 'pair'), may hold values from -2.390625 to 2.390625
- screen: int32 [24, 256], P('aux', 'pair'), may hold values 0 or 1
- factor: float32 [3072, 3072], P('aux', 'pair'), may hold values from -0.109375 to 0.109375
- diag_inv: float32 [3072, 768], P('aux'), may hold values from -2 to 2, as said below
Outputs:
- coulomb: float32 [16, 32768], P(None, ('pair', 'aux'))
The draws below stay inside these ranges and needn't reach their ends.
Inputs may be any that keep to these rules, and one draw needn't show every extreme that they name: `diag_inv`: each block of 768 rows is an upper triangular matrix with a positive diagonal.
All inputs are finite; a program needn't handle non-finite values. No bound on the sum of `screen` on one device may be relied on, other than what follows from the above.
Results may differ from the reference program's by a relative error of at most 0.0041.
Values may be sent and summed in bfloat16 or wider, within the bound.
A program may use at most 128 MiB of HBM per device.

```python
import math
import jax
import jax.numpy as jnp
from jax import lax

AUX_DEV = 384
DENS = 16
TILE = 128
SOLVE_BLOCKS = 4
NAUX = 3072
BLOCK = 768
NPAIR = 32768


def draw_diag_inv(key, part):
    off_key = jax.random.fold_in(key, 11)
    diag_key = jax.random.fold_in(key, 12)
    spread = 0.5 / math.sqrt(BLOCK)
    offdiag = jnp.clip(jax.random.normal(off_key, (NAUX, BLOCK), jnp.float32), -4.0, 4.0) * spread
    diagonal = jnp.exp(jax.random.uniform(diag_key, (NAUX, 1), jnp.float32, math.log(0.7), math.log(1.4)))
    within = (jnp.arange(NAUX, dtype=jnp.int32) % BLOCK)[:, None]
    across = jnp.arange(BLOCK, dtype=jnp.int32)[None, :]
    return jnp.where(across == within, diagonal, jnp.where(across > within, offdiag, 0.0)).astype(jnp.float32)


def set_ends(result, own_key, low, largest):
    extent = result.shape
    index_at = [jax.random.randint(jax.random.fold_in(own_key, axis), (), 0, extent[axis]) for axis in range(len(extent))]
    result = result.at[tuple(index_at)].set(low)
    longest = extent.index(max(extent))
    index_at[longest] = (index_at[longest] + 1) % extent[longest]
    return result.at[tuple(index_at)].set(largest)


def spiked(result, rng, source, target, parts, factor):
    owner, partner = [(jnp.arange(result.shape[axis_at]) // (result.shape[axis_at] // parts)).reshape([-1 if axis == axis_at else 1 for axis in range(result.ndim)]) for axis_at in (source, target)]
    chosen = jax.random.permutation(rng, parts)[partner]
    strong = (owner == chosen) | (owner == (partner + parts // 2) % parts)
    return jnp.where(strong, factor * result, result)


def shard_levels(rng, dims, shards, smallest, high):
    gain = 1.0
    for dim, shards_of in shards:
        heights = jax.random.uniform(jax.random.fold_in(jax.random.fold_in(rng, 6), dim), (shards_of,), jnp.float32, smallest / len(shards), high / len(shards))
        gain = gain * jnp.repeat(jnp.exp(heights), dims[dim] // shards_of).reshape((-1,) + (1,) * (len(dims) - 1 - dim))
    return gain


def noise(rng, extent, width, bound, split=(), held_as=jnp.bfloat16):
    level = shard_levels(rng, extent, split, -0.22, 0.18) if split else 1.0
    array = jax.random.normal(rng, extent, jnp.float32) * width * level
    return jnp.minimum(jnp.maximum(array, -bound), bound).astype(held_as)


def heavy_noise(own_key, dims, width, reach, shards, heavy, kind=jnp.bfloat16):
    entries = width * jax.random.normal(own_key, dims, jnp.float32)
    if shards:
        entries = entries * shard_levels(own_key, dims, shards, -0.22, 0.18)
    return jnp.clip(spiked(entries, jax.random.fold_in(own_key, 3), *heavy), -reach, reach).astype(kind)


def setup_inputs(seed: int = 0) -> dict:
    key_list = jax.random.split(jax.random.key(seed), 6)
    integrals = heavy_noise(key_list[0], (NAUX, NPAIR), NAUX ** -0.5, 0.15625, ((0, 8), (1, 4)), (0, 1, 8, 2.0))
    densities = noise(key_list[1], (DENS, NPAIR), 0.4, 2.390625, ((1, 4),))
    screen = set_ends((jax.random.randint(key_list[2], (NAUX // TILE, NPAIR // TILE), 0, 4) < 3).astype(jnp.int32), jax.random.fold_in(key_list[2], 1), 0, 1)
    factor = noise(key_list[3], (NAUX, NAUX), NAUX ** -0.5, 0.109375, ((0, 8), (1, 4)), jnp.float32)
    diag_inv = draw_diag_inv(jax.random.fold_in(key_list[5], 71), 0)
    return dict(integrals=integrals, densities=densities, screen=screen, factor=factor, diag_inv=diag_inv)


def reference(integrals, densities, screen, factor, diag_inv):
    blocks = NAUX // AUX_DEV
    highest = lax.Precision.HIGHEST
    tiles_block = AUX_DEV // TILE

    def masked_rows(index):
        slab_rows = lax.dynamic_slice_in_dim(integrals, index * AUX_DEV, AUX_DEV, 0)
        screen_tiles = lax.dynamic_slice_in_dim(screen, index * tiles_block, tiles_block, 0)
        expanded = jnp.repeat(jnp.repeat(screen_tiles, TILE, axis=0), TILE, axis=1).astype(jnp.bfloat16)
        return slab_rows * expanded

    def fit_block(index):
        return lax.dot_general(densities, masked_rows(index), (((1,), (1,)), ((), ())), preferred_element_type=jnp.float32)

    fitted_blocks = lax.map(fit_block, jnp.arange(blocks, dtype=jnp.int32))
    fitted = jnp.transpose(fitted_blocks, (1, 0, 2)).reshape(DENS, NAUX)

    solved = jnp.zeros((DENS, NAUX), jnp.float32)
    for k in range(SOLVE_BLOCKS):
        offset = k * BLOCK
        upper = offset + BLOCK
        residual = fitted[:, offset:upper]
        if k > 0:
            residual = residual - jnp.dot(solved[:, :offset], factor[offset:upper, :offset].T, precision=highest, preferred_element_type=jnp.float32)
        solved = solved.at[:, offset:upper].set(jnp.dot(residual, diag_inv[offset:upper], precision=highest, preferred_element_type=jnp.float32))

    coefficients = jnp.zeros((DENS, NAUX), jnp.float32)
    for k in reversed(range(SOLVE_BLOCKS)):
        offset = k * BLOCK
        upper = offset + BLOCK
        residual = solved[:, offset:upper]
        if upper < NAUX:
            residual = residual - jnp.dot(coefficients[:, upper:], factor[upper:, offset:upper], precision=highest, preferred_element_type=jnp.float32)
        coefficients = coefficients.at[:, offset:upper].set(jnp.dot(residual, diag_inv[offset:upper].T, precision=highest, preferred_element_type=jnp.float32))

    rounded = coefficients.astype(jnp.bfloat16)

    def add_block(running, index):
        weights = lax.dynamic_slice_in_dim(rounded, index * AUX_DEV, AUX_DEV, 1)
        return running + jnp.dot(weights, masked_rows(index), preferred_element_type=jnp.float32), None

    coulomb, unused = lax.scan(add_block, jnp.zeros((DENS, NPAIR), jnp.float32), jnp.arange(blocks, dtype=jnp.int32))
    return coulomb
```

```python
import functools

import jax
import jax.numpy as jnp
from jax import lax
from jax.experimental import pallas as pl
from jax.experimental.pallas import tpu as pltpu
from jax.sharding import PartitionSpec as P

TILE = 128
SOLVE_BLOCKS = 4
STREAM = 1024
MESH = pl.DeviceIdType.MESH
NN = (((1,), (0,)), ((), ()))
NT = (((1,), (1,)), ((), ()))
F32 = jnp.float32
BF16 = jnp.bfloat16


def split(values):
    high = values.astype(BF16)
    return high, (values - high.astype(F32)).astype(BF16)


def dot_split(values, high, low, dims):
    top, rest = split(values)
    rows = values.shape[0]
    both = lax.dot_general(
        jnp.concatenate([top, rest], 0), high, dims, preferred_element_type=F32
    )
    minor = lax.dot_general(top, low, dims, preferred_element_type=F32)
    return both[:rows] + (both[rows:] + minor)


def kernel(
    n_aux, n_pair,
    integrals, densities, screen, factor, diag_inv, out,
    masked, dens, fac, inv, fac_hi, fac_lo, inv_hi, inv_lo,
    fit_out, fit_in, u_out, u_in, s_out, s_in, s_sum, own_in, resid, coef, v_out, v_in,
    part_out, part_in,
    load_sem, small_sem,
    fit_send, fit_recv, u_send, u_recv, s_send, s_recv, own_send, own_recv,
    coef_send, coef_recv, v_send, v_recv, part_send, part_recv,
):
    height, width = masked.shape
    breadth = fac.shape[1]
    block = inv.shape[1]
    members = block // height
    group = block // breadth
    pieces = breadth // height
    share = width // n_aux
    chunks = width // STREAM

    row = lax.axis_index("aux")
    col = lax.axis_index("pair")
    mine = row // members
    member = lax.rem(row, members)
    column_block = col // group
    column_part = lax.rem(col, group)

    def home_of(k):
        return jnp.maximum(k - 1, 0) * group

    home = home_of(mine)
    is_home = col == home
    below = column_block < mine

    def remote(src, dst, send, recv, aux, pair):
        return pltpu.make_async_remote_copy(
            src_ref=src, dst_ref=dst, send_sem=send, recv_sem=recv,
            device_id={"aux": aux, "pair": pair}, device_id_type=MESH,
        )

    def load(c):
        at = pl.ds(pl.multiple_of(c * STREAM, STREAM), STREAM)
        return pltpu.make_async_copy(integrals.at[:, at], masked.at[:, at], load_sem.at[c])

    load_dens = pltpu.make_async_copy(densities, dens, small_sem.at[0])
    load_fac = pltpu.make_async_copy(factor, fac, small_sem.at[1])
    load_inv = pltpu.make_async_copy(diag_inv, inv, small_sem.at[2])
    load_dens.start()
    for c in range(chunks):
        load(c).start()
    load_inv.start()

    @pl.when(below)
    def _():
        load_fac.start()

    barrier = pltpu.get_barrier_semaphore()
    everyone = n_aux * n_pair
    me = row * n_pair + col

    def greet(i, carry):
        other = lax.rem(me + i, everyone)
        pl.semaphore_signal(
            barrier, inc=1,
            device_id={"aux": other // n_pair, "pair": lax.rem(other, n_pair)},
            device_id_type=MESH,
        )
        return carry

    lax.fori_loop(1, everyone, greet, 0)
    load_dens.wait()

    def fit_step(c, total):
        load(c).wait()
        base = pl.multiple_of(c * STREAM, STREAM)
        for r in range(height // TILE):
            for t in range(STREAM // TILE):
                flag = screen[r, c * (STREAM // TILE) + t].astype(F32)
                at = (pl.ds(r * TILE, TILE), pl.ds(pl.multiple_of(base + t * TILE, TILE), TILE))
                masked[at] = masked[at] * jnp.full((TILE, TILE), flag, F32).astype(BF16)
        span = pl.ds(base, STREAM)
        return total + lax.dot_general(
            dens[:, span], masked[:, span], NT, preferred_element_type=F32
        )

    fitted = lax.fori_loop(0, chunks, fit_step, jnp.zeros((dens.shape[0], height), F32))
    fit_out[...] = fitted
    pl.semaphore_wait(barrier, everyone - 1)

    send_fit = remote(fit_out, fit_in.at[col], fit_send, fit_recv.at[col], row, home)

    @pl.when(jnp.logical_not(is_home))
    def _():
        send_fit.start()

    load_inv.wait()
    high, low = split(inv[...])
    inv_hi[...] = high
    inv_lo[...] = low

    @pl.when(below)
    def _():
        load_fac.wait()
        high, low = split(fac[...])
        fac_hi[...] = high
        fac_lo[...] = low

    @pl.when(below)
    def _():
        for x in range(pieces):
            whole_x = column_part * pieces + x
            for c in range(members):
                @pl.when(whole_x >= c)
                def _():
                    remote(s_out.at[0], s_in.at[c, x], s_send.at[0, 0], s_recv.at[c, x], row, col).wait_recv()
                    if c == 0:
                        s_sum[x] = s_in[c, x]
                    else:
                        s_sum[x] += s_in[c, x]
        known = jnp.concatenate([s_sum[x] for x in range(pieces)], 1)
        u_out[...] = dot_split(known, fac_hi[...], fac_lo[...], NT)

        @pl.when(jnp.logical_not(is_home))
        def _():
            remote(u_out, u_in.at[col], u_send, u_recv.at[col], row, home).start()

    def send_solved(x, start):
        part, piece = x // pieces, x % pieces

        def later(d, carry):
            copy = remote(
                s_out.at[x], s_in.at[member, piece], s_send.at[x, d],
                s_recv.at[member, piece], d, mine * group + part,
            )
            copy.start() if start else copy.wait_send()
            return carry

        lax.fori_loop((mine + 1) * members, n_aux, later, 0)
        for i in range(1, members):
            other = lax.rem(member + i, members)

            @pl.when(other <= x)
            def _():
                copy = remote(
                    s_out.at[x], own_in.at[member, x], own_send.at[x, i],
                    own_recv.at[member, x], mine * members + other, home,
                )
                copy.start() if start else copy.wait_send()

    @pl.when(is_home)
    def _():
        fit_total = fit_out
        for p in range(n_pair):
            @pl.when(p != home)
            def _():
                remote(fit_out, fit_in.at[p], fit_send, fit_recv.at[p], row, col).wait_recv()
                fit_total[...] += fit_in[p]
        for p in range(n_pair):
            @pl.when(jnp.logical_and(p // group < mine, p != home))
            def _():
                remote(u_out, u_in.at[p], u_send, u_recv.at[p], row, col).wait_recv()
                fit_total[...] -= u_in[p]

        @pl.when(below)
        def _():
            fit_total[...] -= u_out[...]

        for x in range(members):
            @pl.when(x >= member)
            def _():
                at = pl.ds(x * height, height)
                s_out[x] = dot_split(fit_total[...], inv_hi[:, at], inv_lo[:, at], NN)
                send_solved(x, True)

        for x in range(members):
            @pl.when(x >= member)
            def _():
                resid[x] = s_out[x]
                for i in range(1, members):
                    other = lax.rem(member + i, members)

                    @pl.when(other <= x)
                    def _():
                        remote(s_out.at[0], own_in.at[other, x], own_send.at[0, 0], own_recv.at[other, x], row, col).wait_recv()
                        resid[x] += own_in[other, x]

        def subtract(i, carry):
            source = n_aux - 1 - i
            for x in range(members):
                @pl.when(x >= member)
                def _():
                    remote(v_out.at[0], v_in.at[source, x], v_send.at[0, 0], v_recv.at[source, x], row, col).wait_recv()
                    resid[x] -= v_in[source, x]
            return carry

        lax.fori_loop(0, n_aux - (mine + 1) * members, subtract, 0)
        for x in reversed(range(members)):
            @pl.when(x >= member)
            def _():
                at = pl.ds(x * height, height)
                term = dot_split(resid[x], inv_hi[:, at], inv_lo[:, at], NT)
                if x == members - 1:
                    coef[...] = term
                else:
                    coef[...] += term

        for i in range(1, n_pair):
            remote(coef, coef, coef_send.at[i], coef_recv, row, lax.rem(col + i, n_pair)).start()

    @pl.when(jnp.logical_not(is_home))
    def _():
        remote(coef, coef, coef_send.at[0], coef_recv, row, col).wait_recv()

    def send_v(x, start):
        whole_x = column_part * pieces + x
        for c in range(members):
            @pl.when(c <= whole_x)
            def _():
                copy = remote(
                    v_out.at[x], v_in.at[row, whole_x], v_send.at[x, c],
                    v_recv.at[row, whole_x], column_block * members + c, home_of(column_block),
                )
                copy.start() if start else copy.wait_send()

    @pl.when(below)
    def _():
        for x in range(pieces):
            at = pl.ds(x * height, height)
            v_out[x] = dot_split(coef[...], fac_hi[:, at], fac_lo[:, at], NN)
            send_v(x, True)

    rounded = coef[...].astype(BF16)

    def product(target):
        span = pl.ds(pl.multiple_of(target * share, TILE), share)
        return lax.dot_general(rounded, masked[:, span], NN, preferred_element_type=F32)

    def part_copy(i):
        target = lax.rem(row + i, n_aux)
        return target, remote(
            part_out.at[target], part_in.at[row], part_send.at[target], part_recv.at[row], target, col
        )

    def give(i, carry):
        target, copy = part_copy(i)
        part_out[target] = product(target).astype(BF16)
        copy.start()
        return carry

    lax.fori_loop(1, n_aux, give, 0)
    total = product(row)

    def take(i, total):
        source = lax.rem(row + n_aux - i, n_aux)
        remote(part_out.at[0], part_in.at[source], part_send.at[0], part_recv.at[source], row, col).wait_recv()
        return total + part_in[source].astype(F32)

    out[...] = lax.fori_loop(1, n_aux, take, total)

    @pl.when(jnp.logical_not(is_home))
    def _():
        send_fit.wait_send()

        @pl.when(below)
        def _():
            remote(u_out, u_in.at[col], u_send, u_recv.at[col], row, home).wait_send()

    @pl.when(is_home)
    def _():
        for x in range(members):
            @pl.when(x >= member)
            def _():
                send_solved(x, False)
        for i in range(1, n_pair):
            remote(coef, coef, coef_send.at[i], coef_recv, row, lax.rem(col + i, n_pair)).wait_send()

    @pl.when(below)
    def _():
        for x in range(pieces):
            send_v(x, False)

    def sent(i, carry):
        part_copy(i)[1].wait_send()
        return carry

    lax.fori_loop(1, n_aux, sent, 0)


def shards(integrals, densities, screen, factor, diag_inv):
    n_aux, n_pair = lax.axis_size("aux"), lax.axis_size("pair")
    height, width = integrals.shape
    breadth, block = factor.shape[1], diag_inv.shape[1]
    count = densities.shape[0]
    members, pieces = block // height, breadth // height
    share = width // n_aux
    vmem, dma = pltpu.VMEM, pltpu.SemaphoreType.DMA

    def rows(*lead):
        return vmem(lead + (count, height), F32)

    return pl.pallas_call(
        functools.partial(kernel, n_aux, n_pair),
        out_shape=jax.ShapeDtypeStruct((count, share), F32),
        in_specs=[
            pl.BlockSpec(memory_space=pl.ANY),
            pl.BlockSpec(memory_space=pl.ANY),
            pl.BlockSpec(memory_space=pltpu.SMEM),
            pl.BlockSpec(memory_space=pl.ANY),
            pl.BlockSpec(memory_space=pl.ANY),
        ],
        out_specs=pl.BlockSpec(memory_space=pltpu.VMEM),
        scratch_shapes=[
            vmem((height, width), BF16), vmem((count, width), BF16),
            vmem((height, breadth), F32), vmem((height, block), F32),
            vmem((height, breadth), BF16), vmem((height, breadth), BF16),
            vmem((height, block), BF16), vmem((height, block), BF16),
            rows(), rows(n_pair), rows(), rows(n_pair),
            rows(members), rows(members, pieces), rows(pieces), rows(members, members),
            rows(members), rows(), rows(pieces), rows(n_aux, members),
            vmem((n_aux, count, share), BF16), vmem((n_aux, count, share), BF16),
            dma((width // STREAM,)), dma((3,)),
            dma, dma((n_pair,)), dma, dma((n_pair,)),
            dma((members, n_aux)), dma((members, pieces)),
            dma((members, members)), dma((members, members)),
            dma((n_pair,)), dma, dma((pieces, members)), dma((n_aux, members)),
            dma((n_aux,)), dma((n_aux,)),
        ],
        compiler_params=pltpu.CompilerParams(
            collective_id=0, has_side_effects=True, vmem_limit_bytes=60 * 2**20
        ),
    )(integrals, densities, screen, factor, diag_inv)


def solution(mesh):
    in_specs = (
        P("aux", "pair"),
        P(None, "pair"),
        P("aux", "pair"),
        P("aux", "pair"),
        P("aux", None),
    )
    out_specs = P(None, ("pair", "aux"))
    return jax.shard_map(shards, mesh=mesh, in_specs=in_specs, out_specs=out_specs, check_vma=False)
```

```python
import functools

import jax
import jax.numpy as jnp
from jax import lax
from jax.experimental import pallas as pl
from jax.experimental.pallas import tpu as pltpu
from jax.sharding import PartitionSpec as P

TILE = 128
SOLVE_BLOCKS = 4
STREAM = 1024
VMEM_ROOM = 48 * 2**20
MESH = pl.DeviceIdType.MESH
NN = (((1,), (0,)), ((), ()))
NT = (((1,), (1,)), ((), ()))
F32 = jnp.float32
BF16 = jnp.bfloat16


def split(values):
    high = values.astype(BF16)
    return high, (values - high.astype(F32)).astype(BF16)


def dot_split(values, high, low, dims):
    top, rest = split(values)
    rows = values.shape[0]
    both = lax.dot_general(
        jnp.concatenate([top, rest], 0), high, dims, preferred_element_type=F32
    )
    minor = lax.dot_general(top, low, dims, preferred_element_type=F32)
    return both[:rows] + (both[rows:] + minor)


def spread_kernel(
    n_aux, n_pair,
    integrals, densities, screen, factor, diag_inv, out,
    masked, dens, fac, inv, fac_hi, fac_lo, inv_hi, inv_lo,
    fit_out, fit_in, u_out, u_in, s_out, s_in, s_sum, own_in, resid, coef, v_out, v_in,
    part_out, part_in,
    load_sem, small_sem,
    fit_send, fit_recv, u_send, u_recv, s_send, s_recv, own_send, own_recv,
    coef_send, coef_recv, v_send, v_recv, part_send, part_recv,
):
    height, width = masked.shape
    breadth = fac.shape[1]
    block = inv.shape[1]
    members = block // height
    group = block // breadth
    pieces = breadth // height
    share = width // n_aux
    chunks = width // STREAM

    row = lax.axis_index("aux")
    col = lax.axis_index("pair")
    mine = row // members
    member = lax.rem(row, members)
    column_block = col // group
    column_part = lax.rem(col, group)

    def home_of(k):
        return jnp.maximum(k - 1, 0) * group

    home = home_of(mine)
    is_home = col == home
    below = column_block < mine

    def remote(src, dst, send, recv, aux, pair):
        return pltpu.make_async_remote_copy(
            src_ref=src, dst_ref=dst, send_sem=send, recv_sem=recv,
            device_id={"aux": aux, "pair": pair}, device_id_type=MESH,
        )

    def load(c):
        at = pl.ds(pl.multiple_of(c * STREAM, STREAM), STREAM)
        return pltpu.make_async_copy(integrals.at[:, at], masked.at[:, at], load_sem.at[c])

    load_dens = pltpu.make_async_copy(densities, dens, small_sem.at[0])
    load_fac = pltpu.make_async_copy(factor, fac, small_sem.at[1])
    load_inv = pltpu.make_async_copy(diag_inv, inv, small_sem.at[2])
    load_dens.start()
    for c in range(chunks):
        load(c).start()
    load_inv.start()

    @pl.when(below)
    def _():
        load_fac.start()

    barrier = pltpu.get_barrier_semaphore()
    everyone = n_aux * n_pair
    me = row * n_pair + col

    def greet(i, carry):
        other = lax.rem(me + i, everyone)
        pl.semaphore_signal(
            barrier, inc=1,
            device_id={"aux": other // n_pair, "pair": lax.rem(other, n_pair)},
            device_id_type=MESH,
        )
        return carry

    lax.fori_loop(1, everyone, greet, 0)
    load_dens.wait()

    def fit_step(c, total):
        load(c).wait()
        base = pl.multiple_of(c * STREAM, STREAM)
        for r in range(height // TILE):
            for t in range(STREAM // TILE):
                flag = screen[r, c * (STREAM // TILE) + t].astype(F32)
                at = (pl.ds(r * TILE, TILE), pl.ds(pl.multiple_of(base + t * TILE, TILE), TILE))
                masked[at] = masked[at] * jnp.full((TILE, TILE), flag, F32).astype(BF16)
        span = pl.ds(base, STREAM)
        return total + lax.dot_general(
            dens[:, span], masked[:, span], NT, preferred_element_type=F32
        )

    fitted = lax.fori_loop(0, chunks, fit_step, jnp.zeros((dens.shape[0], height), F32))
    fit_out[...] = fitted
    pl.semaphore_wait(barrier, everyone - 1)

    send_fit = remote(fit_out, fit_in.at[col], fit_send, fit_recv.at[col], row, home)

    @pl.when(jnp.logical_not(is_home))
    def _():
        send_fit.start()

    load_inv.wait()
    high, low = split(inv[...])
    inv_hi[...] = high
    inv_lo[...] = low

    @pl.when(below)
    def _():
        load_fac.wait()
        high, low = split(fac[...])
        fac_hi[...] = high
        fac_lo[...] = low

    @pl.when(below)
    def _():
        for x in range(pieces):
            whole_x = column_part * pieces + x
            for c in range(members):
                @pl.when(whole_x >= c)
                def _():
                    remote(s_out.at[0], s_in.at[c, x], s_send.at[0, 0], s_recv.at[c, x], row, col).wait_recv()
                    if c == 0:
                        s_sum[x] = s_in[c, x]
                    else:
                        s_sum[x] += s_in[c, x]
        known = jnp.concatenate([s_sum[x] for x in range(pieces)], 1)
        u_out[...] = dot_split(known, fac_hi[...], fac_lo[...], NT)

        @pl.when(jnp.logical_not(is_home))
        def _():
            remote(u_out, u_in.at[col], u_send, u_recv.at[col], row, home).start()

    def send_solved(x, start):
        part, piece = x // pieces, x % pieces

        def later(d, carry):
            copy = remote(
                s_out.at[x], s_in.at[member, piece], s_send.at[x, d],
                s_recv.at[member, piece], d, mine * group + part,
            )
            copy.start() if start else copy.wait_send()
            return carry

        lax.fori_loop((mine + 1) * members, n_aux, later, 0)
        for i in range(1, members):
            other = lax.rem(member + i, members)

            @pl.when(other <= x)
            def _():
                copy = remote(
                    s_out.at[x], own_in.at[member, x], own_send.at[x, i],
                    own_recv.at[member, x], mine * members + other, home,
                )
                copy.start() if start else copy.wait_send()

    @pl.when(is_home)
    def _():
        fit_total = fit_out
        for p in range(n_pair):
            @pl.when(p != home)
            def _():
                remote(fit_out, fit_in.at[p], fit_send, fit_recv.at[p], row, col).wait_recv()
                fit_total[...] += fit_in[p]
        for p in range(n_pair):
            @pl.when(jnp.logical_and(p // group < mine, p != home))
            def _():
                remote(u_out, u_in.at[p], u_send, u_recv.at[p], row, col).wait_recv()
                fit_total[...] -= u_in[p]

        @pl.when(below)
        def _():
            fit_total[...] -= u_out[...]

        for x in range(members):
            @pl.when(x >= member)
            def _():
                at = pl.ds(x * height, height)
                s_out[x] = dot_split(fit_total[...], inv_hi[:, at], inv_lo[:, at], NN)
                send_solved(x, True)

        for x in range(members):
            @pl.when(x >= member)
            def _():
                resid[x] = s_out[x]
                for i in range(1, members):
                    other = lax.rem(member + i, members)

                    @pl.when(other <= x)
                    def _():
                        remote(s_out.at[0], own_in.at[other, x], own_send.at[0, 0], own_recv.at[other, x], row, col).wait_recv()
                        resid[x] += own_in[other, x]

        def subtract(i, carry):
            source = n_aux - 1 - i
            for x in range(members):
                @pl.when(x >= member)
                def _():
                    remote(v_out.at[0], v_in.at[source, x], v_send.at[0, 0], v_recv.at[source, x], row, col).wait_recv()
                    resid[x] -= v_in[source, x]
            return carry

        lax.fori_loop(0, n_aux - (mine + 1) * members, subtract, 0)
        for x in reversed(range(members)):
            @pl.when(x >= member)
            def _():
                at = pl.ds(x * height, height)
                term = dot_split(resid[x], inv_hi[:, at], inv_lo[:, at], NT)
                if x == members - 1:
                    coef[...] = term
                else:
                    coef[...] += term

        for i in range(1, n_pair):
            remote(coef, coef, coef_send.at[i], coef_recv, row, lax.rem(col + i, n_pair)).start()

    @pl.when(jnp.logical_not(is_home))
    def _():
        remote(coef, coef, coef_send.at[0], coef_recv, row, col).wait_recv()

    def send_v(x, start):
        whole_x = column_part * pieces + x
        for c in range(members):
            @pl.when(c <= whole_x)
            def _():
                copy = remote(
                    v_out.at[x], v_in.at[row, whole_x], v_send.at[x, c],
                    v_recv.at[row, whole_x], column_block * members + c, home_of(column_block),
                )
                copy.start() if start else copy.wait_send()

    @pl.when(below)
    def _():
        for x in range(pieces):
            at = pl.ds(x * height, height)
            v_out[x] = dot_split(coef[...], fac_hi[:, at], fac_lo[:, at], NN)
            send_v(x, True)

    rounded = coef[...].astype(BF16)

    def product(target):
        span = pl.ds(pl.multiple_of(target * share, TILE), share)
        return lax.dot_general(rounded, masked[:, span], NN, preferred_element_type=F32)

    def part_copy(i):
        target = lax.rem(row + i, n_aux)
        return target, remote(
            part_out.at[target], part_in.at[row], part_send.at[target], part_recv.at[row], target, col
        )

    def give(i, carry):
        target, copy = part_copy(i)
        part_out[target] = product(target).astype(BF16)
        copy.start()
        return carry

    lax.fori_loop(1, n_aux, give, 0)
    total = product(row)

    def take(i, total):
        source = lax.rem(row + n_aux - i, n_aux)
        remote(part_out.at[0], part_in.at[source], part_send.at[0], part_recv.at[source], row, col).wait_recv()
        return total + part_in[source].astype(F32)

    out[...] = lax.fori_loop(1, n_aux, take, total)

    @pl.when(jnp.logical_not(is_home))
    def _():
        send_fit.wait_send()

        @pl.when(below)
        def _():
            remote(u_out, u_in.at[col], u_send, u_recv.at[col], row, home).wait_send()

    @pl.when(is_home)
    def _():
        for x in range(members):
            @pl.when(x >= member)
            def _():
                send_solved(x, False)
        for i in range(1, n_pair):
            remote(coef, coef, coef_send.at[i], coef_recv, row, lax.rem(col + i, n_pair)).wait_send()

    @pl.when(below)
    def _():
        for x in range(pieces):
            send_v(x, False)

    def sent(i, carry):
        part_copy(i)[1].wait_send()
        return carry

    lax.fori_loop(1, n_aux, sent, 0)


def lead_kernel(
    n_aux, n_pair,
    integrals, densities, screen, factor, diag_inv, out,
    masked, dens, fac, inv, fac_hi, fac_lo, inv_hi, inv_lo, step_hi, step_lo,
    fit_out, fit_in, u_out, u_in, s_in, s_own, resid, coef, rounded, v_out, v_in,
    part_out, part_in,
    load_sem, small_sem, fac_send, fac_recv, inv_send, inv_recv,
    fit_send, fit_recv, u_send, u_recv, s_send, s_recv,
    coef_send, coef_recv, round_send, round_recv, v_send, v_recv, part_send, part_recv,
):
    height, width = masked.shape
    block = inv.shape[1]
    members = block // height
    share = width // n_aux
    chunks = width // STREAM

    row = lax.axis_index("aux")
    col = lax.axis_index("pair")
    mine = row // members
    member = lax.rem(row, members)
    lead = members - 1
    lead_row = mine * members + lead
    is_lead = member == lead

    def home_of(k):
        return jnp.maximum(k - 1, 0)

    home = home_of(mine)
    at_home = col == home
    below = col < mine
    lead_home = jnp.logical_and(is_lead, at_home)
    lead_below = jnp.logical_and(is_lead, below)
    lead_aside = jnp.logical_and(lead_below, col != home)

    def remote(src, dst, send, recv, aux, pair):
        return pltpu.make_async_remote_copy(
            src_ref=src, dst_ref=dst, send_sem=send, recv_sem=recv,
            device_id={"aux": aux, "pair": pair}, device_id_type=MESH,
        )

    def load(c):
        at = pl.ds(pl.multiple_of(c * STREAM, STREAM), STREAM)
        return pltpu.make_async_copy(integrals.at[:, at], masked.at[:, at], load_sem.at[c])

    own = pl.ds(lead * height, height)
    load_dens = pltpu.make_async_copy(densities, dens, small_sem.at[0])
    load_fac = pltpu.make_async_copy(factor, fac.at[own], small_sem.at[1])
    load_inv = pltpu.make_async_copy(diag_inv, inv.at[own], small_sem.at[2])

    def move_fac(c):
        return remote(factor, fac.at[pl.ds(c * height, height)], fac_send, fac_recv.at[c], lead_row, col)

    def move_inv(c):
        right = pl.ds(c * height, block - c * height)
        return remote(
            diag_inv.at[:, right], inv.at[pl.ds(c * height, height), right],
            inv_send, inv_recv.at[c], lead_row, col,
        )

    barrier = pltpu.get_barrier_semaphore()
    everyone = n_aux * n_pair
    me = row * n_pair + col

    def greet(i, carry):
        other = lax.rem(me + i, everyone)
        pl.semaphore_signal(
            barrier, inc=1,
            device_id={"aux": other // n_pair, "pair": lax.rem(other, n_pair)},
            device_id_type=MESH,
        )
        return carry

    lax.fori_loop(1, everyone, greet, 0)
    load_dens.start()
    for c in range(chunks):
        load(c).start()

    @pl.when(lead_home)
    def _():
        load_inv.start()
        for c in range(1, lead):
            inv[pl.ds(c * height, height), pl.ds(0, c * height)] = jnp.zeros((height, c * height), F32)

    @pl.when(lead_below)
    def _():
        load_fac.start()

    pl.semaphore_wait(barrier, everyone - 1)
    for c in range(lead):
        @pl.when(member == c)
        def _():
            @pl.when(at_home)
            def _():
                move_inv(c).start()

            @pl.when(below)
            def _():
                move_fac(c).start()

    load_dens.wait()

    def fit_step(c, total):
        load(c).wait()
        base = pl.multiple_of(c * STREAM, STREAM)
        for r in range(height // TILE):
            for t in range(STREAM // TILE):
                flag = screen[r, c * (STREAM // TILE) + t].astype(F32)
                at = (pl.ds(r * TILE, TILE), pl.ds(pl.multiple_of(base + t * TILE, TILE), TILE))
                masked[at] = masked[at] * jnp.full((TILE, TILE), flag, F32).astype(BF16)
        span = pl.ds(base, STREAM)
        return total + lax.dot_general(
            dens[:, span], masked[:, span], NT, preferred_element_type=F32
        )

    fit_out[...] = lax.fori_loop(0, chunks, fit_step, jnp.zeros((dens.shape[0], height), F32))

    send_fit = remote(
        fit_out, fit_in.at[col, member], fit_send, fit_recv.at[col, member], lead_row, home
    )

    @pl.when(jnp.logical_not(lead_home))
    def _():
        send_fit.start()

    @pl.when(lead_home)
    def _():
        load_inv.wait()
        for c in range(lead):
            move_inv(c).wait_recv()
        inv_hi[...], inv_lo[...] = split(inv[...])

    @pl.when(lead_below)
    def _():
        load_fac.wait()
        for c in range(lead):
            move_fac(c).wait_recv()

    @pl.when(lead_aside)
    def _():
        fac_hi[...], fac_lo[...] = split(fac[...])

    @pl.when(jnp.logical_and(lead_home, below))
    def _():
        high, low = split(fac[...].T)
        fac_hi[...] = high
        fac_lo[...] = low
        whole = lax.dot_general(fac_hi[...], inv_hi[...], NN, preferred_element_type=F32)
        whole += lax.dot_general(fac_lo[...], inv_hi[...], NN, preferred_element_type=F32)
        whole += lax.dot_general(fac_hi[...], inv_lo[...], NN, preferred_element_type=F32)
        step_hi[...], step_lo[...] = split(whole)

    recv_s = remote(s_own, s_in, s_send.at[0], s_recv, row, col)

    @pl.when(lead_aside)
    def _():
        recv_s.wait_recv()
        u_out[...] = dot_split(s_in[...], fac_hi[...], fac_lo[...], NT)
        remote(u_out, u_in.at[col], u_send, u_recv.at[col], row, home).start()

    def send_solved(start):
        def later(k, carry):
            copy = remote(s_own, s_in, s_send.at[k], s_recv, k * members + lead, mine)
            copy.start() if start else copy.wait_send()
            return carry

        lax.fori_loop(mine + 1, SOLVE_BLOCKS, later, 0)

    def send_rounded(start):
        for c in range(members):
            for i in range(n_pair):
                def one():
                    copy = remote(
                        rounded.at[c], rounded.at[c], round_send.at[c, i], round_recv,
                        mine * members + c, lax.rem(col + i, n_pair),
                    )
                    copy.start() if start else copy.wait_send()

                if c != lead or i:
                    one()

    def send_coef(start):
        for p in range(n_pair):
            @pl.when(p < mine - 1)
            def _():
                copy = remote(coef, coef, coef_send.at[p], coef_recv, row, p)
                copy.start() if start else copy.wait_send()

    send_v = remote(
        v_out, v_in.at[mine], v_send, v_recv.at[mine], col * members + lead, home_of(col)
    )

    @pl.when(lead_home)
    def _():
        resid[:, own] = fit_out[...]
        for p in range(n_pair):
            for c in range(members):
                if c != lead:
                    @pl.when(p == home)
                    def _():
                        remote(fit_out, fit_in.at[p, c], fit_send, fit_recv.at[p, c], row, col).wait_recv()
                        resid[:, pl.ds(c * height, height)] = fit_in[p, c]
        for p in range(n_pair):
            for c in range(members):
                @pl.when(p != home)
                def _():
                    remote(fit_out, fit_in.at[p, c], fit_send, fit_recv.at[p, c], row, col).wait_recv()
                    resid[:, pl.ds(c * height, height)] += fit_in[p, c]
        for p in range(n_pair):
            @pl.when(p < mine - 1)
            def _():
                remote(u_out, u_in.at[p], u_send, u_recv.at[p], row, col).wait_recv()
                resid[...] -= u_in[p]
        s_own[...] = dot_split(resid[...], inv_hi[...], inv_lo[...], NN)

        @pl.when(below)
        def _():
            recv_s.wait_recv()
            s_own[...] -= dot_split(s_in[...], step_hi[...], step_lo[...], NN)

        send_solved(True)

        resid[...] = s_own[...]

        def subtract(i, carry):
            source = SOLVE_BLOCKS - 1 - i
            remote(v_out, v_in.at[source], v_send, v_recv.at[source], row, col).wait_recv()
            resid[...] -= v_in[source]
            return carry

        lax.fori_loop(0, SOLVE_BLOCKS - 1 - mine, subtract, 0)

        @pl.when(below)
        def _():
            v_out[...] = dot_split(resid[...], step_hi[...], step_lo[...], NT)
            send_v.start()

        coef[...] = dot_split(resid[...], inv_hi[...], inv_lo[...], NT)
        for c in range(members):
            rounded[c] = coef[:, pl.ds(c * height, height)].astype(BF16)
        send_coef(True)
        send_rounded(True)

    @pl.when(lead_aside)
    def _():
        remote(coef, coef, coef_send.at[0], coef_recv, row, col).wait_recv()
        v_out[...] = dot_split(coef[...], fac_hi[...], fac_lo[...], NN)
        send_v.start()

    @pl.when(jnp.logical_not(lead_home))
    def _():
        remote(rounded.at[0], rounded.at[0], round_send.at[0, 0], round_recv, row, col).wait_recv()

    mine_rounded = rounded[member]

    def product(target):
        span = pl.ds(pl.multiple_of(target * share, TILE), share)
        return lax.dot_general(mine_rounded, masked[:, span], NN, preferred_element_type=F32)

    def part_copy(i):
        target = lax.rem(row + i, n_aux)
        return target, remote(
            part_out.at[target], part_in.at[row], part_send.at[target], part_recv.at[row], target, col
        )

    def give(i, carry):
        target, copy = part_copy(i)
        part_out[target] = product(target).astype(BF16)
        copy.start()
        return carry

    lax.fori_loop(1, n_aux, give, 0)
    total = product(row)

    def take(i, total):
        source = lax.rem(row + n_aux - i, n_aux)
        remote(part_out.at[0], part_in.at[source], part_send.at[0], part_recv.at[source], row, col).wait_recv()
        return total + part_in[source].astype(F32)

    out[...] = lax.fori_loop(1, n_aux, take, total)

    for c in range(lead):
        @pl.when(member == c)
        def _():
            @pl.when(at_home)
            def _():
                move_inv(c).wait_send()

            @pl.when(below)
            def _():
                move_fac(c).wait_send()

    @pl.when(jnp.logical_not(lead_home))
    def _():
        send_fit.wait_send()

    @pl.when(lead_aside)
    def _():
        remote(u_out, u_in.at[col], u_send, u_recv.at[col], row, home).wait_send()

    @pl.when(lead_below)
    def _():
        send_v.wait_send()

    @pl.when(lead_home)
    def _():
        send_solved(False)
        send_coef(False)
        send_rounded(False)

    def sent(i, carry):
        part_copy(i)[1].wait_send()
        return carry

    lax.fori_loop(1, n_aux, sent, 0)


def shards(integrals, densities, screen, factor, diag_inv):
    n_aux, n_pair = lax.axis_size("aux"), lax.axis_size("pair")
    height, width = integrals.shape
    breadth, block = factor.shape[1], diag_inv.shape[1]
    count = densities.shape[0]
    members, pieces = block // height, breadth // height
    share = width // n_aux
    vmem, dma = pltpu.VMEM, pltpu.SemaphoreType.DMA

    def rows(*lead):
        return vmem(lead + (count, height), F32)

    def whole(*lead):
        return vmem(lead + (count, block), F32)

    weights = 2 * block * block * 4 + 6 * block * block * 2
    if breadth == block and weights + integrals.size * 2 <= VMEM_ROOM:
        body = lead_kernel
        scratch = [
            vmem((height, width), BF16), vmem((count, width), BF16),
            vmem((block, block), F32), vmem((block, block), F32),
            *[vmem((block, block), BF16) for _ in range(6)],
            rows(), rows(n_pair, members), whole(), whole(n_pair), whole(), whole(), whole(), whole(),
            vmem((members, count, height), BF16), whole(), whole(SOLVE_BLOCKS),
            vmem((n_aux, count, share), BF16), vmem((n_aux, count, share), BF16),
            dma((width // STREAM,)), dma((3,)),
            dma, dma((members,)), dma, dma((members,)),
            dma, dma((n_pair, members)), dma, dma((n_pair,)), dma((SOLVE_BLOCKS,)), dma,
            dma((n_pair,)), dma, dma((members, n_pair)), dma, dma, dma((SOLVE_BLOCKS,)),
            dma((n_aux,)), dma((n_aux,)),
        ]
    else:
        body = spread_kernel
        scratch = [
            vmem((height, width), BF16), vmem((count, width), BF16),
            vmem((height, breadth), F32), vmem((height, block), F32),
            vmem((height, breadth), BF16), vmem((height, breadth), BF16),
            vmem((height, block), BF16), vmem((height, block), BF16),
            rows(), rows(n_pair), rows(), rows(n_pair),
            rows(members), rows(members, pieces), rows(pieces), rows(members, members),
            rows(members), rows(), rows(pieces), rows(n_aux, members),
            vmem((n_aux, count, share), BF16), vmem((n_aux, count, share), BF16),
            dma((width // STREAM,)), dma((3,)),
            dma, dma((n_pair,)), dma, dma((n_pair,)),
            dma((members, n_aux)), dma((members, pieces)),
            dma((members, members)), dma((members, members)),
            dma((n_pair,)), dma, dma((pieces, members)), dma((n_aux, members)),
            dma((n_aux,)), dma((n_aux,)),
        ]
    return pl.pallas_call(
        functools.partial(body, n_aux, n_pair),
        out_shape=jax.ShapeDtypeStruct((count, share), F32),
        in_specs=[
            pl.BlockSpec(memory_space=pl.ANY),
            pl.BlockSpec(memory_space=pl.ANY),
            pl.BlockSpec(memory_space=pltpu.SMEM),
            pl.BlockSpec(memory_space=pl.ANY),
            pl.BlockSpec(memory_space=pl.ANY),
        ],
        out_specs=pl.BlockSpec(memory_space=pltpu.VMEM),
        scratch_shapes=scratch,
        compiler_params=pltpu.CompilerParams(
            collective_id=0, has_side_effects=True, vmem_limit_bytes=60 * 2**20
        ),
    )(integrals, densities, screen, factor, diag_inv)


def solution(mesh):
    in_specs = (
        P("aux", "pair"),
        P(None, "pair"),
        P("aux", "pair"),
        P("aux", "pair"),
        P("aux", None),
    )
    out_specs = P(None, ("pair", "aux"))
    return jax.shard_map(shards, mesh=mesh, in_specs=in_specs, out_specs=out_specs, check_vma=False)
```

```python
import functools

import jax
import jax.numpy as jnp
from jax import lax
from jax.experimental import pallas as pl
from jax.experimental.pallas import tpu as pltpu
from jax.sharding import PartitionSpec as P

TILE = 128
SOLVE_BLOCKS = 4
STREAM = 1024
VMEM_ROOM = 48 * 2**20
MESH = pl.DeviceIdType.MESH
NN = (((1,), (0,)), ((), ()))
NT = (((1,), (1,)), ((), ()))
F32 = jnp.float32
BF16 = jnp.bfloat16


def split(values):
    high = values.astype(BF16)
    return high, (values - high.astype(F32)).astype(BF16)


def dot_split(values, high, low, dims):
    top, rest = split(values)
    rows = values.shape[0]
    both = lax.dot_general(
        jnp.concatenate([top, rest], 0), high, dims, preferred_element_type=F32
    )
    minor = lax.dot_general(top, low, dims, preferred_element_type=F32)
    return both[:rows] + (both[rows:] + minor)


def spread_kernel(
    n_aux, n_pair,
    integrals, densities, screen, factor, diag_inv, out,
    masked, dens, fac, inv, fac_hi, fac_lo, inv_hi, inv_lo,
    fit_out, fit_in, u_out, u_in, s_out, s_in, s_sum, own_in, resid, coef, v_out, v_in,
    part_out, part_in,
    load_sem, small_sem,
    fit_send, fit_recv, u_send, u_recv, s_send, s_recv, own_send, own_recv,
    coef_send, coef_recv, v_send, v_recv, part_send, part_recv,
):
    height, width = masked.shape
    breadth = fac.shape[1]
    block = inv.shape[1]
    members = block // height
    group = block // breadth
    pieces = breadth // height
    share = width // n_aux
    chunks = width // STREAM

    row = lax.axis_index("aux")
    col = lax.axis_index("pair")
    mine = row // members
    member = lax.rem(row, members)
    column_block = col // group
    column_part = lax.rem(col, group)

    def home_of(k):
        return jnp.maximum(k - 1, 0) * group

    home = home_of(mine)
    is_home = col == home
    below = column_block < mine

    def remote(src, dst, send, recv, aux, pair):
        return pltpu.make_async_remote_copy(
            src_ref=src, dst_ref=dst, send_sem=send, recv_sem=recv,
            device_id={"aux": aux, "pair": pair}, device_id_type=MESH,
        )

    def load(c):
        at = pl.ds(pl.multiple_of(c * STREAM, STREAM), STREAM)
        return pltpu.make_async_copy(integrals.at[:, at], masked.at[:, at], load_sem.at[c])

    load_dens = pltpu.make_async_copy(densities, dens, small_sem.at[0])
    load_fac = pltpu.make_async_copy(factor, fac, small_sem.at[1])
    load_inv = pltpu.make_async_copy(diag_inv, inv, small_sem.at[2])
    load_dens.start()
    for c in range(chunks):
        load(c).start()
    load_inv.start()

    @pl.when(below)
    def _():
        load_fac.start()

    barrier = pltpu.get_barrier_semaphore()
    everyone = n_aux * n_pair
    me = row * n_pair + col

    def greet(i, carry):
        other = lax.rem(me + i, everyone)
        pl.semaphore_signal(
            barrier, inc=1,
            device_id={"aux": other // n_pair, "pair": lax.rem(other, n_pair)},
            device_id_type=MESH,
        )
        return carry

    lax.fori_loop(1, everyone, greet, 0)
    load_dens.wait()

    def fit_step(c, total):
        load(c).wait()
        base = pl.multiple_of(c * STREAM, STREAM)
        for r in range(height // TILE):
            for t in range(STREAM // TILE):
                flag = screen[r, c * (STREAM // TILE) + t].astype(F32)
                at = (pl.ds(r * TILE, TILE), pl.ds(pl.multiple_of(base + t * TILE, TILE), TILE))
                masked[at] = masked[at] * jnp.full((TILE, TILE), flag, F32).astype(BF16)
        span = pl.ds(base, STREAM)
        return total + lax.dot_general(
            dens[:, span], masked[:, span], NT, preferred_element_type=F32
        )

    fitted = lax.fori_loop(0, chunks, fit_step, jnp.zeros((dens.shape[0], height), F32))
    fit_out[...] = fitted
    pl.semaphore_wait(barrier, everyone - 1)

    send_fit = remote(fit_out, fit_in.at[col], fit_send, fit_recv.at[col], row, home)

    @pl.when(jnp.logical_not(is_home))
    def _():
        send_fit.start()

    load_inv.wait()
    high, low = split(inv[...])
    inv_hi[...] = high
    inv_lo[...] = low

    @pl.when(below)
    def _():
        load_fac.wait()
        high, low = split(fac[...])
        fac_hi[...] = high
        fac_lo[...] = low

    @pl.when(below)
    def _():
        for x in range(pieces):
            whole_x = column_part * pieces + x
            for c in range(members):
                @pl.when(whole_x >= c)
                def _():
                    remote(s_out.at[0], s_in.at[c, x], s_send.at[0, 0], s_recv.at[c, x], row, col).wait_recv()
                    if c == 0:
                        s_sum[x] = s_in[c, x]
                    else:
                        s_sum[x] += s_in[c, x]
        known = jnp.concatenate([s_sum[x] for x in range(pieces)], 1)
        u_out[...] = dot_split(known, fac_hi[...], fac_lo[...], NT)

        @pl.when(jnp.logical_not(is_home))
        def _():
            remote(u_out, u_in.at[col], u_send, u_recv.at[col], row, home).start()

    def send_solved(x, start):
        part, piece = x // pieces, x % pieces

        def later(d, carry):
            copy = remote(
                s_out.at[x], s_in.at[member, piece], s_send.at[x, d],
                s_recv.at[member, piece], d, mine * group + part,
            )
            copy.start() if start else copy.wait_send()
            return carry

        lax.fori_loop((mine + 1) * members, n_aux, later, 0)
        for i in range(1, members):
            other = lax.rem(member + i, members)

            @pl.when(other <= x)
            def _():
                copy = remote(
                    s_out.at[x], own_in.at[member, x], own_send.at[x, i],
                    own_recv.at[member, x], mine * members + other, home,
                )
                copy.start() if start else copy.wait_send()

    @pl.when(is_home)
    def _():
        fit_total = fit_out
        for p in range(n_pair):
            @pl.when(p != home)
            def _():
                remote(fit_out, fit_in.at[p], fit_send, fit_recv.at[p], row, col).wait_recv()
                fit_total[...] += fit_in[p]
        for p in range(n_pair):
            @pl.when(jnp.logical_and(p // group < mine, p != home))
            def _():
                remote(u_out, u_in.at[p], u_send, u_recv.at[p], row, col).wait_recv()
                fit_total[...] -= u_in[p]

        @pl.when(below)
        def _():
            fit_total[...] -= u_out[...]

        for x in range(members):
            @pl.when(x >= member)
            def _():
                at = pl.ds(x * height, height)
                s_out[x] = dot_split(fit_total[...], inv_hi[:, at], inv_lo[:, at], NN)
                send_solved(x, True)

        for x in range(members):
            @pl.when(x >= member)
            def _():
                resid[x] = s_out[x]
                for i in range(1, members):
                    other = lax.rem(member + i, members)

                    @pl.when(other <= x)
                    def _():
                        remote(s_out.at[0], own_in.at[other, x], own_send.at[0, 0], own_recv.at[other, x], row, col).wait_recv()
                        resid[x] += own_in[other, x]

        def subtract(i, carry):
            source = n_aux - 1 - i
            for x in range(members):
                @pl.when(x >= member)
                def _():
                    remote(v_out.at[0], v_in.at[source, x], v_send.at[0, 0], v_recv.at[source, x], row, col).wait_recv()
                    resid[x] -= v_in[source, x]
            return carry

        lax.fori_loop(0, n_aux - (mine + 1) * members, subtract, 0)
        for x in reversed(range(members)):
            @pl.when(x >= member)
            def _():
                at = pl.ds(x * height, height)
                term = dot_split(resid[x], inv_hi[:, at], inv_lo[:, at], NT)
                if x == members - 1:
                    coef[...] = term
                else:
                    coef[...] += term

        for i in range(1, n_pair):
            remote(coef, coef, coef_send.at[i], coef_recv, row, lax.rem(col + i, n_pair)).start()

    @pl.when(jnp.logical_not(is_home))
    def _():
        remote(coef, coef, coef_send.at[0], coef_recv, row, col).wait_recv()

    def send_v(x, start):
        whole_x = column_part * pieces + x
        for c in range(members):
            @pl.when(c <= whole_x)
            def _():
                copy = remote(
                    v_out.at[x], v_in.at[row, whole_x], v_send.at[x, c],
                    v_recv.at[row, whole_x], column_block * members + c, home_of(column_block),
                )
                copy.start() if start else copy.wait_send()

    @pl.when(below)
    def _():
        for x in range(pieces):
            at = pl.ds(x * height, height)
            v_out[x] = dot_split(coef[...], fac_hi[:, at], fac_lo[:, at], NN)
            send_v(x, True)

    rounded = coef[...].astype(BF16)

    def product(target):
        span = pl.ds(pl.multiple_of(target * share, TILE), share)
        return lax.dot_general(rounded, masked[:, span], NN, preferred_element_type=F32)

    def part_copy(i):
        target = lax.rem(row + i, n_aux)
        return target, remote(
            part_out.at[target], part_in.at[row], part_send.at[target], part_recv.at[row], target, col
        )

    def give(i, carry):
        target, copy = part_copy(i)
        part_out[target] = product(target).astype(BF16)
        copy.start()
        return carry

    lax.fori_loop(1, n_aux, give, 0)
    total = product(row)

    def take(i, total):
        source = lax.rem(row + n_aux - i, n_aux)
        remote(part_out.at[0], part_in.at[source], part_send.at[0], part_recv.at[source], row, col).wait_recv()
        return total + part_in[source].astype(F32)

    out[...] = lax.fori_loop(1, n_aux, take, total)

    @pl.when(jnp.logical_not(is_home))
    def _():
        send_fit.wait_send()

        @pl.when(below)
        def _():
            remote(u_out, u_in.at[col], u_send, u_recv.at[col], row, home).wait_send()

    @pl.when(is_home)
    def _():
        for x in range(members):
            @pl.when(x >= member)
            def _():
                send_solved(x, False)
        for i in range(1, n_pair):
            remote(coef, coef, coef_send.at[i], coef_recv, row, lax.rem(col + i, n_pair)).wait_send()

    @pl.when(below)
    def _():
        for x in range(pieces):
            send_v(x, False)

    def sent(i, carry):
        part_copy(i)[1].wait_send()
        return carry

    lax.fori_loop(1, n_aux, sent, 0)


def lead_kernel(
    n_aux, n_pair,
    integrals, densities, screen, factor, diag_inv, out,
    masked, dens, fac, inv, fac_hi, fac_lo, inv_hi, inv_lo, step_hi, step_lo,
    inv_t_hi, inv_t_lo, step_t_hi, step_t_lo,
    fit_out, fit_in, u_out, u_in, s_in, s_own, resid, coef, rounded, v_out, v_in,
    part_out, part_in,
    load_sem, small_sem, fac_send, fac_recv, inv_send, inv_recv,
    fit_send, fit_recv, u_send, u_recv, s_send, s_recv,
    coef_send, coef_recv, round_send, round_recv, v_send, v_recv, part_send, part_recv,
):
    height, width = masked.shape
    block = inv.shape[1]
    members = block // height
    share = width // n_aux
    chunks = width // STREAM

    row = lax.axis_index("aux")
    col = lax.axis_index("pair")
    mine = row // members
    member = lax.rem(row, members)
    lead = members - 1
    lead_row = mine * members + lead
    is_lead = member == lead

    def home_of(k):
        return jnp.maximum(k - 1, 0)

    home = home_of(mine)
    at_home = col == home
    below = col < mine
    lead_home = jnp.logical_and(is_lead, at_home)
    lead_below = jnp.logical_and(is_lead, below)
    lead_aside = jnp.logical_and(lead_below, col != home)

    def remote(src, dst, send, recv, aux, pair):
        return pltpu.make_async_remote_copy(
            src_ref=src, dst_ref=dst, send_sem=send, recv_sem=recv,
            device_id={"aux": aux, "pair": pair}, device_id_type=MESH,
        )

    def load(c):
        at = pl.ds(pl.multiple_of(c * STREAM, STREAM), STREAM)
        return pltpu.make_async_copy(integrals.at[:, at], masked.at[:, at], load_sem.at[c])

    own = pl.ds(lead * height, height)
    load_dens = pltpu.make_async_copy(densities, dens, small_sem.at[0])
    load_fac = pltpu.make_async_copy(factor, fac.at[own], small_sem.at[1])
    load_inv = pltpu.make_async_copy(diag_inv, inv.at[own], small_sem.at[2])

    def move_fac(c):
        return remote(factor, fac.at[pl.ds(c * height, height)], fac_send, fac_recv.at[c], lead_row, col)

    def move_inv(c):
        right = pl.ds(c * height, block - c * height)
        return remote(
            diag_inv.at[:, right], inv.at[pl.ds(c * height, height), right],
            inv_send, inv_recv.at[c], lead_row, col,
        )

    load_dens.start()
    for c in range(chunks):
        load(c).start()

    @pl.when(lead_home)
    def _():
        load_inv.start()
        for c in range(1, lead):
            inv[pl.ds(c * height, height), pl.ds(0, c * height)] = jnp.zeros((height, c * height), F32)

    @pl.when(lead_below)
    def _():
        load_fac.start()

    barrier = pltpu.get_barrier_semaphore()

    def greet(aux, pair):
        pl.semaphore_signal(
            barrier, inc=1, device_id={"aux": aux, "pair": pair}, device_id_type=MESH
        )

    aside = jnp.logical_and(is_lead, jnp.logical_and(col >= 1, below))
    for i in range(1, n_aux):
        greet(lax.rem(row + i, n_aux), col)

    @pl.when(lead_home)
    def _():
        for c in range(members):
            for i in range(1, n_pair):
                greet(mine * members + c, lax.rem(col + i, n_pair))

    @pl.when(jnp.logical_not(at_home))
    def _():
        greet(lead_row, home)

    for k in range(1, SOLVE_BLOCKS):
        @pl.when(jnp.logical_and(lead_home, jnp.logical_and(mine >= 1, k > mine)))
        def _():
            greet(k * members + lead, mine)

    @pl.when(aside)
    def _():
        greet(col * members + lead, home_of(col))

    greeted = (
        n_aux - 1
        + jnp.where(lead_home, members * (n_pair - 1), 0)
        + jnp.where(at_home, 0, 1)
        + jnp.where(jnp.logical_and(lead_home, mine >= 1), SOLVE_BLOCKS - 1 - mine, 0)
        + jnp.where(aside, 1, 0)
    )
    pl.semaphore_wait(barrier, greeted)
    for c in range(lead):
        @pl.when(member == c)
        def _():
            @pl.when(at_home)
            def _():
                move_inv(c).start()

            @pl.when(below)
            def _():
                move_fac(c).start()

    load_dens.wait()

    def fit_step(c, total):
        load(c).wait()
        base = pl.multiple_of(c * STREAM, STREAM)
        for r in range(height // TILE):
            for t in range(STREAM // TILE):
                flag = screen[r, c * (STREAM // TILE) + t].astype(F32)
                at = (pl.ds(r * TILE, TILE), pl.ds(pl.multiple_of(base + t * TILE, TILE), TILE))
                masked[at] = masked[at] * jnp.full((TILE, TILE), flag, F32).astype(BF16)
        span = pl.ds(base, STREAM)
        return total + lax.dot_general(
            dens[:, span], masked[:, span], NT, preferred_element_type=F32
        )

    fit_out[...] = lax.fori_loop(0, chunks, fit_step, jnp.zeros((dens.shape[0], height), F32))

    send_fit = remote(
        fit_out, fit_in.at[col, member], fit_send, fit_recv.at[col, member], lead_row, home
    )

    @pl.when(jnp.logical_not(lead_home))
    def _():
        send_fit.start()

    @pl.when(lead_home)
    def _():
        load_inv.wait()
        for c in range(lead):
            move_inv(c).wait_recv()
        inv_hi[...], inv_lo[...] = split(inv[...])
        inv_t_hi[...], inv_t_lo[...] = split(inv[...].T)

    @pl.when(lead_below)
    def _():
        load_fac.wait()
        for c in range(lead):
            move_fac(c).wait_recv()

    @pl.when(lead_aside)
    def _():
        fac_hi[...], fac_lo[...] = split(fac[...])

    @pl.when(jnp.logical_and(lead_home, below))
    def _():
        high, low = split(fac[...].T)
        fac_hi[...] = high
        fac_lo[...] = low
        whole = lax.dot_general(fac_hi[...], inv_hi[...], NN, preferred_element_type=F32)
        whole += lax.dot_general(fac_lo[...], inv_hi[...], NN, preferred_element_type=F32)
        whole += lax.dot_general(fac_hi[...], inv_lo[...], NN, preferred_element_type=F32)
        step_hi[...], step_lo[...] = split(whole)
        step_t_hi[...], step_t_lo[...] = split(whole.T)

    recv_s = remote(s_own, s_in, s_send.at[0], s_recv, row, col)

    @pl.when(lead_aside)
    def _():
        recv_s.wait_recv()
        u_out[...] = dot_split(s_in[...], fac_hi[...], fac_lo[...], NT)
        remote(u_out, u_in.at[col], u_send, u_recv.at[col], row, home).start()

    def send_solved(start):
        def later(k, carry):
            copy = remote(s_own, s_in, s_send.at[k], s_recv, k * members + lead, mine)
            copy.start() if start else copy.wait_send()
            return carry

        lax.fori_loop(mine + 1, SOLVE_BLOCKS, later, 0)

    def send_rounded(start):
        for c in range(members):
            for i in range(n_pair):
                def one():
                    copy = remote(
                        rounded.at[c], rounded.at[c], round_send.at[c, i], round_recv,
                        mine * members + c, lax.rem(col + i, n_pair),
                    )
                    copy.start() if start else copy.wait_send()

                if c != lead or i:
                    one()

    def send_coef(start):
        for p in range(n_pair):
            @pl.when(p < mine - 1)
            def _():
                copy = remote(coef, coef, coef_send.at[p], coef_recv, row, p)
                copy.start() if start else copy.wait_send()

    send_v = remote(
        v_out, v_in.at[mine], v_send, v_recv.at[mine], col * members + lead, home_of(col)
    )

    @pl.when(lead_home)
    def _():
        resid[:, own] = fit_out[...]
        for p in range(n_pair):
            for c in range(members):
                if c != lead:
                    @pl.when(p == home)
                    def _():
                        remote(fit_out, fit_in.at[p, c], fit_send, fit_recv.at[p, c], row, col).wait_recv()
                        resid[:, pl.ds(c * height, height)] = fit_in[p, c]
        for p in range(n_pair):
            for c in range(members):
                @pl.when(p != home)
                def _():
                    remote(fit_out, fit_in.at[p, c], fit_send, fit_recv.at[p, c], row, col).wait_recv()
                    resid[:, pl.ds(c * height, height)] += fit_in[p, c]
        for p in range(n_pair):
            @pl.when(p < mine - 1)
            def _():
                remote(u_out, u_in.at[p], u_send, u_recv.at[p], row, col).wait_recv()
                resid[...] -= u_in[p]
        s_own[...] = dot_split(resid[...], inv_hi[...], inv_lo[...], NN)

        @pl.when(below)
        def _():
            recv_s.wait_recv()
            s_own[...] -= dot_split(s_in[...], step_hi[...], step_lo[...], NN)

        send_solved(True)

        resid[...] = s_own[...]

        def subtract(i, carry):
            source = SOLVE_BLOCKS - 1 - i
            remote(v_out, v_in.at[source], v_send, v_recv.at[source], row, col).wait_recv()
            resid[...] -= v_in[source]
            return carry

        lax.fori_loop(0, SOLVE_BLOCKS - 1 - mine, subtract, 0)

        @pl.when(below)
        def _():
            v_out[...] = dot_split(resid[...], step_t_hi[...], step_t_lo[...], NN)
            send_v.start()

        coef[...] = dot_split(resid[...], inv_t_hi[...], inv_t_lo[...], NN)
        for c in range(members):
            rounded[c] = coef[:, pl.ds(c * height, height)].astype(BF16)
        send_coef(True)
        send_rounded(True)

    @pl.when(lead_aside)
    def _():
        remote(coef, coef, coef_send.at[0], coef_recv, row, col).wait_recv()
        v_out[...] = dot_split(coef[...], fac_hi[...], fac_lo[...], NN)
        send_v.start()

    @pl.when(jnp.logical_not(lead_home))
    def _():
        remote(rounded.at[0], rounded.at[0], round_send.at[0, 0], round_recv, row, col).wait_recv()

    mine_rounded = rounded[member]

    def product(target):
        span = pl.ds(pl.multiple_of(target * share, TILE), share)
        return lax.dot_general(mine_rounded, masked[:, span], NN, preferred_element_type=F32)

    def part_copy(i):
        target = lax.rem(row + n_aux - i, n_aux)
        return target, remote(
            part_out.at[target], part_in.at[row], part_send.at[target], part_recv.at[row], target, col
        )

    def give(i, carry):
        target, copy = part_copy(i)
        part_out[target] = product(target).astype(BF16)
        copy.start()
        return carry

    lax.fori_loop(1, n_aux, give, 0)
    total = product(row)

    def take(i, total):
        source = lax.rem(row + i, n_aux)
        remote(part_out.at[0], part_in.at[source], part_send.at[0], part_recv.at[source], row, col).wait_recv()
        return total + part_in[source].astype(F32)

    out[...] = lax.fori_loop(1, n_aux, take, total)

    for c in range(lead):
        @pl.when(member == c)
        def _():
            @pl.when(at_home)
            def _():
                move_inv(c).wait_send()

            @pl.when(below)
            def _():
                move_fac(c).wait_send()

    @pl.when(jnp.logical_not(lead_home))
    def _():
        send_fit.wait_send()

    @pl.when(lead_aside)
    def _():
        remote(u_out, u_in.at[col], u_send, u_recv.at[col], row, home).wait_send()

    @pl.when(lead_below)
    def _():
        send_v.wait_send()

    @pl.when(lead_home)
    def _():
        send_solved(False)
        send_coef(False)
        send_rounded(False)

    def sent(i, carry):
        part_copy(i)[1].wait_send()
        return carry

    lax.fori_loop(1, n_aux, sent, 0)


def shards(integrals, densities, screen, factor, diag_inv):
    n_aux, n_pair = lax.axis_size("aux"), lax.axis_size("pair")
    height, width = integrals.shape
    breadth, block = factor.shape[1], diag_inv.shape[1]
    count = densities.shape[0]
    members, pieces = block // height, breadth // height
    share = width // n_aux
    vmem, dma = pltpu.VMEM, pltpu.SemaphoreType.DMA

    def rows(*lead):
        return vmem(lead + (count, height), F32)

    def whole(*lead):
        return vmem(lead + (count, block), F32)

    weights = 2 * block * block * 4 + 10 * block * block * 2
    if breadth == block and weights + integrals.size * 2 <= VMEM_ROOM:
        body = lead_kernel
        scratch = [
            vmem((height, width), BF16), vmem((count, width), BF16),
            vmem((block, block), F32), vmem((block, block), F32),
            *[vmem((block, block), BF16) for _ in range(10)],
            rows(), rows(n_pair, members), whole(), whole(n_pair), whole(), whole(), whole(), whole(),
            vmem((members, count, height), BF16), whole(), whole(SOLVE_BLOCKS),
            vmem((n_aux, count, share), BF16), vmem((n_aux, count, share), BF16),
            dma((width // STREAM,)), dma((3,)),
            dma, dma((members,)), dma, dma((members,)),
            dma, dma((n_pair, members)), dma, dma((n_pair,)), dma((SOLVE_BLOCKS,)), dma,
            dma((n_pair,)), dma, dma((members, n_pair)), dma, dma, dma((SOLVE_BLOCKS,)),
            dma((n_aux,)), dma((n_aux,)),
        ]
    else:
        body = spread_kernel
        scratch = [
            vmem((height, width), BF16), vmem((count, width), BF16),
            vmem((height, breadth), F32), vmem((height, block), F32),
            vmem((height, breadth), BF16), vmem((height, breadth), BF16),
            vmem((height, block), BF16), vmem((height, block), BF16),
            rows(), rows(n_pair), rows(), rows(n_pair),
            rows(members), rows(members, pieces), rows(pieces), rows(members, members),
            rows(members), rows(), rows(pieces), rows(n_aux, members),
            vmem((n_aux, count, share), BF16), vmem((n_aux, count, share), BF16),
            dma((width // STREAM,)), dma((3,)),
            dma, dma((n_pair,)), dma, dma((n_pair,)),
            dma((members, n_aux)), dma((members, pieces)),
            dma((members, members)), dma((members, members)),
            dma((n_pair,)), dma, dma((pieces, members)), dma((n_aux, members)),
            dma((n_aux,)), dma((n_aux,)),
        ]
    return pl.pallas_call(
        functools.partial(body, n_aux, n_pair),
        out_shape=jax.ShapeDtypeStruct((count, share), F32),
        in_specs=[
            pl.BlockSpec(memory_space=pl.ANY),
            pl.BlockSpec(memory_space=pl.ANY),
            pl.BlockSpec(memory_space=pltpu.SMEM),
            pl.BlockSpec(memory_space=pl.ANY),
            pl.BlockSpec(memory_space=pl.ANY),
        ],
        out_specs=pl.BlockSpec(memory_space=pltpu.VMEM),
        scratch_shapes=scratch,
        compiler_params=pltpu.CompilerParams(
            collective_id=0, has_side_effects=True, vmem_limit_bytes=60 * 2**20
        ),
    )(integrals, densities, screen, factor, diag_inv)


def solution(mesh):
    in_specs = (
        P("aux", "pair"),
        P(None, "pair"),
        P("aux", "pair"),
        P("aux", "pair"),
        P("aux", None),
    )
    out_specs = P(None, ("pair", "aux"))
    return jax.shard_map(shards, mesh=mesh, in_specs=in_specs, out_specs=out_specs, check_vma=False)
```
